32 devices in a mesh: dom: 8 (over y, x, core), shift: 4 (over z).
Axes of the slice: x: 2, y: 2, z: 4, core: 2. Of those that a mesh axis runs over, the one named last changes fastest.
Arguments:
- sources: float32 [32, 32, 16, 128], P('shift', 'dom'), may hold values from -6 to 6
- kappa: float32 [32, 16, 128], P('dom'), may hold values from 0 to 2
- mass: float32 [32, 16, 128], P('dom'), may hold values from 0.25 to 4
- shift_table: float32 [64], replicated, may hold values from 0.5 to 4
- shift_ids: int32 [16], P('shift'), may hold values from 0 to 63
- sketch: bfloat16 [1024, 32, 16, 128], P(None, 'dom'), may hold values from -0.1875 to 0.1875
Outputs:
- solution: float32 [16, 32, 32, 16, 128], P('shift', None, 'dom')
- residual: float32 [16, 32, 32, 16, 128], P('shift', None, 'dom')
The draws below stay inside these ranges and needn't reach their ends.
Inputs may be any that keep to these rules, and one draw needn't show every extreme that they name: `shift_ids`: index into shift_table.
All inputs are finite; a program needn't handle non-finite values.
Results may differ from the reference program's by a relative error of at most 0.0026.
Values sent between devices are 32-bit elements; how exact they have to be, the bound alone decides.
A program may use at most 128 MiB of HBM per device.

```python
import math
import jax
import jax.numpy as jnp
from jax import lax

SK = 1024
SHIFTS = 16
TABLE = 64
NY = 16
NZ = 128
B = 32
NX = 32


def plant(array, stream_key, least, top_value):
    dims = array.shape
    place = [jax.random.randint(jax.random.fold_in(stream_key, axis), (), 0, dims[axis]) for axis in range(len(dims))]
    array = array.at[tuple(place)].set(least)
    longest = dims.index(max(dims))
    place[longest] = (place[longest] + 1) % dims[longest]
    return array.at[tuple(place)].set(top_value)


def block_scale(own_key, shape, cuts, least, largest):
    gain, own = 1.0, jax.random.fold_in(own_key, 6)
    for dim, blocks in cuts:
        steps = jnp.exp(jax.random.uniform(jax.random.fold_in(own, dim), (blocks,), jnp.float32, least / len(cuts), largest / len(cuts)))
        gain = gain * jnp.repeat(steps, shape[dim] // blocks).reshape([-1 if axis == dim else 1 for axis in range(len(shape))])
    return gain


def gaussian(key, shape, deviation, reach, pieces=(), held_as=jnp.bfloat16):
    drawn = jax.random.normal(key, shape, jnp.float32) * deviation
    if len(pieces) > 0:
        drawn = block_scale(key, shape, pieces, -0.22, 0.18) * drawn
    return jnp.clip(drawn, min=-reach, max=reach).astype(held_as)


def setup_inputs(seed: int = 0) -> dict:
    splits = jax.random.split(jax.random.key(seed), 7)
    return {
        "sources": gaussian(splits[0], (B, NX, NY, NZ), 1.0, 6.0, ((0, 4), (1, 8)), jnp.float32),
        "kappa": jnp.clip(2.0 * jax.random.uniform(splits[1], (NX, NY, NZ), jnp.float32) ** block_scale(splits[1], (NX, NY, NZ), ((0, 8),), -0.2, 0.2), 0.0, 2.0),
        "mass": jnp.clip(jnp.exp(math.log(4.0) - 2.7725887 * jax.random.uniform(splits[2], (NX, NY, NZ), jnp.float32) ** block_scale(splits[2], (NX, NY, NZ), ((0, 8),), -0.2, 0.2)), 0.25, 4.0),
        "shift_table": jnp.clip(jax.random.uniform(splits[3], (TABLE,), jnp.float32, 0.5, 4.0), 0.5, 4.0),
        "shift_ids": plant(jax.random.randint(splits[4], (SHIFTS,), 0, TABLE), jax.random.fold_in(splits[4], 1), 0, TABLE - 1).astype(jnp.int32),
        "sketch": gaussian(splits[5], (SK, NX, NY, NZ), SK ** -0.5, 0.1875, ((1, 8),)),
    }


def shift_values(shift_table, shift_ids):
    entries = jnp.arange(shift_table.shape[0], dtype=jnp.int32)
    picked = jnp.where(shift_ids[:, None] == entries[None, :], shift_table[None, :], 0.0)
    return lax.optimization_barrier(jnp.sum(picked, axis=1))

def apply_operator(field, diag):
    padded = jnp.pad(field, ((0, 0), (1, 1), (1, 1), (1, 1)))
    beside = padded[:, 2:, 1:-1, 1:-1] + padded[:, :-2, 1:-1, 1:-1]
    beside = beside + padded[:, 1:-1, 2:, 1:-1] + padded[:, 1:-1, :-2, 1:-1]
    beside = beside + padded[:, 1:-1, 1:-1, 2:] + padded[:, 1:-1, 1:-1, :-2]
    return diag * field - beside

def solve_small(gram):
    h_vals = [gram[:, 1 + i, 0] for i in range(3)]
    ridge = 0.001 * (gram[:, 1, 1] + gram[:, 2, 2] + gram[:, 3, 3]) / 3.0 + 1.0
    entry = [[gram[:, 1 + i, 1 + k] + (ridge if i == k else 0.0) for k in range(3)] for i in range(3)]
    l00 = jnp.sqrt(entry[0][0])
    l10 = entry[1][0] / l00
    l20 = entry[2][0] / l00
    l11 = jnp.sqrt(entry[1][1] - l10 * l10)
    l21 = (entry[2][1] - l20 * l10) / l11
    l22 = jnp.sqrt(entry[2][2] - l20 * l20 - l21 * l21)
    f0 = h_vals[0] / l00
    f1 = (h_vals[1] - l10 * f0) / l11
    f2 = (h_vals[2] - l20 * f0 - l21 * f1) / l22
    c2 = f2 / l22
    c1 = (f1 - l21 * c2) / l11
    c0 = (f0 - l10 * c1 - l20 * c2) / l00
    return (c0, c1, c2)

def gram_of(sketched):
    return jnp.einsum('rib,rkb->bik', sketched, sketched, precision=lax.Precision.HIGHEST)

def reference(sources, kappa, mass, shift_table, shift_ids, sketch):
    sigma = shift_values(shift_table, shift_ids)
    matrix = sketch.reshape(sketch.shape[0], -1)
    count = sources.shape[0]

    def one_shift(value):
        diag = (6.0 - kappa + value * mass)[None]
        center = 6.0 + value
        w0 = sources
        z0 = apply_operator(w0, diag)
        w1 = (z0 - center * w0) / 6.0
        z1 = apply_operator(w1, diag)
        w2 = (z1 - center * w1) / 6.0
        z2 = apply_operator(w2, diag)
        stacked = jnp.stack([w0, z0, z1, z2], axis=0).astype(jnp.bfloat16).reshape(4 * count, -1)
        sketched = lax.dot_general(matrix, stacked, (((1,), (1,)), ((), ())), preferred_element_type=jnp.float32)
        gram = gram_of(sketched.reshape(matrix.shape[0], 4, count))
        c0, c1, c2 = solve_small(gram)
        c0 = c0[:, None, None, None]
        c1 = c1[:, None, None, None]
        c2 = c2[:, None, None, None]
        solution = c0 * w0 + c1 * w1 + c2 * w2
        residual = w0 - c0 * z0 - c1 * z1 - c2 * z2
        return (solution, residual)
    solution, residual = lax.map(one_shift, sigma)
    return (solution, residual)
```

```python
import functools

import jax
import jax.numpy as jnp
from jax import lax
from jax.experimental import pallas as pl
from jax.experimental.pallas import tpu as pltpu
from jax.sharding import PartitionSpec as P

HALO = 3
STEPS = 4
LANES = 128
MID = 2.25
BASIS = 10
WEIGHTS = 6
IMAGES = ((1, 2), (3, 4, 5), (6, 7, 8, 9))
PAIRS = [(i, k) for i in range(BASIS) for k in range(i, BASIS)]
PAIR_INDEX = {pair: n for n, pair in enumerate(PAIRS)}


def neighbour_sum(field):
    inner = field[1:-1]
    shape = inner.shape
    total = field[2:] + field[:-2]
    for dim in (1, 2):
        size = shape[dim]
        place = lax.broadcasted_iota(jnp.int32, shape, dim)
        total = total + jnp.where(place > 0, pltpu.roll(inner, 1, dim), 0.0)
        total = total + jnp.where(place < size - 1, pltpu.roll(inner, size - 1, dim), 0.0)
    return total


def plane_mask(shape, width, low, high):
    plane = lax.broadcasted_iota(jnp.int32, shape, 0)
    return jnp.where(plane < width, low, jnp.where(plane >= shape[0] - width, high, 1.0))


def edge_flags():
    me = lax.axis_index("dom")
    last = lax.axis_size("dom") - 1
    return (me > 0).astype(jnp.float32), (me < last).astype(jnp.float32)


def basis_fields(w0, diag, mass, mask1, mask2):
    sixth = 1.0 / 6.0
    center = 6.0 + MID
    d1, m1 = diag[1:-1], mass[1:-1]
    d2, m2 = diag[2:-2], mass[2:-2]
    d3, m3 = diag[3:-3], mass[3:-3]
    w0i = w0[1:-1]
    a0 = d1 * w0i - neighbour_sum(w0)
    a1 = m1 * w0i
    scaled1 = sixth * mask1
    g0 = (a0 - center * w0i) * scaled1
    g1 = (a1 - w0i) * scaled1
    g0i, g1i = g0[1:-1], g1[1:-1]
    b0 = d2 * g0i - neighbour_sum(g0)
    b1 = d2 * g1i - neighbour_sum(g1) + m2 * g0i
    b2 = m2 * g1i
    scaled2 = sixth * mask2
    h0 = (b0 - center * g0i) * scaled2
    h1 = (b1 - center * g1i - g0i) * scaled2
    h2 = (b2 - g1i) * scaled2
    h0i, h1i, h2i = h0[1:-1], h1[1:-1], h2[1:-1]
    e0 = d3 * h0i - neighbour_sum(h0)
    e1 = d3 * h1i - neighbour_sum(h1) + m3 * h0i
    e2 = d3 * h2i - neighbour_sum(h2) + m3 * h1i
    e3 = m3 * h2i
    return [
        w0[3:-3], a0[2:-2], a1[2:-2], b0[1:-1], b1[1:-1], b2[1:-1], e0, e1, e2, e3
    ]


def solve_small(h_vals, entry):
    l00 = jnp.sqrt(entry[0][0])
    l10 = entry[1][0] / l00
    l20 = entry[2][0] / l00
    l11 = jnp.sqrt(entry[1][1] - l10 * l10)
    l21 = (entry[2][1] - l20 * l10) / l11
    l22 = jnp.sqrt(entry[2][2] - l20 * l20 - l21 * l21)
    f0 = h_vals[0] / l00
    f1 = (h_vals[1] - l10 * f0) / l11
    f2 = (h_vals[2] - l20 * f0 - l21 * f1) / l22
    c2 = f2 / l22
    c1 = (f1 - l21 * c2) / l11
    c0 = (f0 - l10 * c1 - l20 * c2) / l00
    return (c0, c1, c2)


def coefficients(gram, tau):
    def product(left, right):
        by_degree = {}
        for p, i in enumerate(left):
            for q, k in enumerate(right):
                n = PAIR_INDEX[(min(i, k), max(i, k))]
                column = gram[:, n : n + 1]
                by_degree[p + q] = by_degree[p + q] + column if p + q in by_degree else column
        top = max(by_degree)
        total = jnp.broadcast_to(by_degree[top], (gram.shape[0], LANES))
        for degree in range(top - 1, -1, -1):
            total = total * tau + by_degree[degree]
        return total

    h_vals = [product(image, (0,)) for image in IMAGES]
    entry = [[None] * 3 for _ in range(3)]
    for i in range(3):
        for k in range(i + 1):
            entry[i][k] = product(IMAGES[i], IMAGES[k])
    ridge = 0.001 * (entry[0][0] + entry[1][1] + entry[2][2]) / 3.0 + 1.0
    for i in range(3):
        entry[i][i] = entry[i][i] + ridge
    return solve_small(h_vals, entry)


def weights(solved, tau):
    c0, c1, c2 = solved
    shifted = 6.0 + MID + tau
    of_z1 = c2 * (1.0 / 6.0)
    of_z0 = (c1 - of_z1 * shifted) * (1.0 / 6.0)
    of_w0 = c0 - of_z0 * shifted
    return (of_w0, of_z0, of_z1, c0, c1, c2)


def project_kernel(
    n, groups, src_hbm, kappa_hbm, mass_hbm, table_ref, ids_ref, sketch_ref,
    image_ref, c_ref,
    wide_ref, coeff_ref, rows_buf, mat_ref, raw_ref, fields_ref, out_buf, in_buf, total_ref, gram_all,
    gram_rows, load_sem, in_sem, z_send, z_recv, halo_send, halo_recv, km_send, km_recv,
    rs_send, rs_recv, g_send, g_recv,
):
    me = lax.axis_index("dom")
    group = lax.axis_index("shift")
    nb = wide_ref.shape[1]
    slab = wide_ref.shape[2] - 2 * HALO
    tail = wide_ref.shape[3:]
    shifts = ids_ref.shape[0]
    columns = BASIS * nb
    rows = mat_ref.shape[0]
    blocks, block = rows_buf.shape[0], rows_buf.shape[1]
    steps = out_buf.shape[0]
    stride = rows // steps
    parts = stride // LANES
    chunk = rows // (n // nb)
    turns = chunk // stride
    right, left = lax.rem(me + 1, n), lax.rem(me + n - 1, n)
    has_right, has_left = me < n - 1, me > 0
    has_up, has_down = group < groups - 1, group > 0
    upper = (2 * group) // groups
    nearer = group + upper * (groups - 1 - 2 * group)

    def remote(src, dst, send, recv, **where):
        return pltpu.make_async_remote_copy(
            src_ref=src, dst_ref=dst, send_sem=send, recv_sem=recv,
            device_id=where, device_id_type=pl.DeviceIdType.MESH,
        )

    def load(t):
        return pltpu.make_async_copy(
            sketch_ref.at[pl.ds(t * block, block)], rows_buf.at[t], load_sem.at[t]
        )

    barrier = pltpu.get_barrier_semaphore()
    for t in range(1, n):
        pl.semaphore_signal(
            barrier, inc=1, device_id={"dom": lax.rem(me + t, n)},
            device_id_type=pl.DeviceIdType.MESH,
        )
    for t in range(1, groups):
        pl.semaphore_signal(
            barrier, inc=1, device_id={"shift": lax.rem(group + t, groups)},
            device_id_type=pl.DeviceIdType.MESH,
        )
    inner = pl.ds(HALO, slab)
    arguments = [
        pltpu.make_async_copy(src_hbm, wide_ref.at[group, :, inner], in_sem.at[0]),
        pltpu.make_async_copy(kappa_hbm, coeff_ref.at[0, inner], in_sem.at[1]),
        pltpu.make_async_copy(mass_hbm, coeff_ref.at[1, inner], in_sem.at[2]),
    ]
    for copy in arguments:
        copy.start()
    for t in range(blocks):
        load(t).start()

    @pl.when(jnp.logical_not(has_left))
    def _():
        wide_ref[:, :, pl.ds(0, HALO)] = jnp.zeros((groups, nb, HALO) + tail, jnp.float32)
        coeff_ref[:, pl.ds(0, HALO)] = jnp.zeros((2, HALO) + tail, jnp.float32)

    @pl.when(jnp.logical_not(has_right))
    def _():
        wide_ref[:, :, pl.ds(slab + HALO, HALO)] = jnp.zeros(
            (groups, nb, HALO) + tail, jnp.float32
        )
        coeff_ref[:, pl.ds(slab + HALO, HALO)] = jnp.zeros((2, HALO) + tail, jnp.float32)

    for copy in arguments:
        copy.wait()
    pl.semaphore_wait(barrier, n - 1 + groups - 1)

    def sides(side):
        if side == 0:
            return pl.ds(slab, HALO), pl.ds(0, HALO), right
        return pl.ds(HALO, HALO), pl.ds(slab + HALO, HALO), left

    def halo(slot, side):
        first, target, there = sides(side)
        return remote(
            wide_ref.at[slot, :, first], wide_ref.at[slot, :, target],
            halo_send.at[slot, side], halo_recv.at[slot, side], dom=there,
        )

    def coeff_halo(which, side):
        first, target, there = sides(side)
        return remote(
            coeff_ref.at[which, first], coeff_ref.at[which, target], km_send.at[which, side],
            km_recv.at[which, side], dom=there,
        )

    def across(slot, way):
        return remote(
            wide_ref.at[slot, :, inner], wide_ref.at[slot, :, inner],
            z_send.at[slot, way], z_recv.at[slot],
            shift=group + 1 - 2 * way,
        )

    def other(i):
        if i == 0:
            return group
        longer = 1 - 2 * upper
        both = (2 * nearer - i + groups) // groups
        swing = longer * ((i + 1) // 2) * (1 if i % 2 else -1)
        return group + both * swing + (1 - both) * longer * (i - nearer)

    def to_right(act):
        pl.when(has_right)(act)

    def to_left(act):
        pl.when(has_left)(act)

    def up_from(slot):
        return jnp.logical_and(slot <= group, has_up)

    def down_from(slot):
        return jnp.logical_and(slot >= group, has_down)

    @pl.when(has_right)
    def _():
        halo(group, 0).start()
        for which in range(2):
            coeff_halo(which, 0).start()

    @pl.when(has_left)
    def _():
        halo(group, 1).start()
        for which in range(2):
            coeff_halo(which, 1).start()

    @pl.when(has_up)
    def _():
        across(group, 0).start()

    @pl.when(has_down)
    def _():
        across(group, 1).start()

    def settle(t, carry):
        load(t).wait()
        mat_ref[pl.ds(pl.multiple_of(t * block, block), block)] = rows_buf[t].reshape(
            block, mat_ref.shape[1]
        )
        return carry

    lax.fori_loop(0, blocks, settle, 0)

    @pl.when(has_left)
    def _():
        halo(group, 0).wait_recv()
        for which in range(2):
            coeff_halo(which, 0).wait_recv()

    @pl.when(has_right)
    def _():
        halo(group, 1).wait_recv()
        for which in range(2):
            coeff_halo(which, 1).wait_recv()

    def forward(i):
        slot = other(i)
        across(slot, 0).wait_recv()

        @pl.when(up_from(slot))
        def _():
            across(slot, 0).start()

        @pl.when(down_from(slot))
        def _():
            across(slot, 1).start()

        @pl.when(has_right)
        def _():
            halo(slot, 0).start()

        @pl.when(has_left)
        def _():
            halo(slot, 1).start()

    def settled(i):
        slot = other(i)

        @pl.when(has_left)
        def _():
            halo(slot, 0).wait_recv()

        @pl.when(has_right)
        def _():
            halo(slot, 1).wait_recv()

    low, high = edge_flags()
    planes = slab + 2 * HALO

    def basis_of(slot, b):
        mass = coeff_ref[1]
        diag = (6.0 - coeff_ref[0]) + MID * mass
        mask1 = plane_mask((planes - 2,) + tail, 2, low, high)
        mask2 = plane_mask((planes - 4,) + tail, 1, low, high)
        return basis_fields(wide_ref[slot, b], diag, mass, mask1, mask2)

    def one_source(b, carry):
        for k, field in enumerate(basis_of(group, b)):
            rounded = field.astype(jnp.bfloat16)
            raw_ref[b * BASIS + k] = rounded
            raw_ref[columns + b * BASIS + k] = (field - rounded.astype(jnp.float32)).astype(
                jnp.bfloat16
            )
        return carry

    lax.fori_loop(0, nb, one_source, 0)
    fields_ref[...] = raw_ref[...].reshape(fields_ref.shape)

    def images_of(slot):
        def one(b, carry):
            w0, a0, a1, b0, b1, b2, e0, e1, e2, e3 = basis_of(slot, b)
            place = slot * nb + b
            image_ref[0, place] = w0
            for j in range(shifts):
                tau = table_ref[ids_ref[j]] - MID
                image_ref[1 + j, place] = a0 + tau * a1
                image_ref[1 + shifts + j, place] = b0 + tau * (b1 + tau * b2)
                image_ref[1 + 2 * shifts + j, place] = e0 + tau * (e1 + tau * (e2 + tau * e3))
            return carry

        lax.fori_loop(0, nb, one, 0)

    def scatter(u, there):
        turn = lax.rem(u, turns)
        return remote(
            out_buf.at[u, pl.ds(lax.rem(there, nb) * BASIS, BASIS)],
            in_buf.at[me, :, pl.ds(turn * parts, parts)],
            rs_send.at[u, lax.rem(there, nb)], rs_recv.at[me, turn], dom=there,
        )

    def gathered(source, turn):
        return remote(
            out_buf.at[turn, pl.ds(0, BASIS)],
            in_buf.at[source, :, pl.ds(turn * parts, parts)],
            rs_send.at[turn, 0], rs_recv.at[source, turn], dom=source,
        )

    def each_target(u, act):
        base = (u // turns) * nb
        for t in range(1, nb + 1):
            there = base + lax.rem(me + t, nb)

            @pl.when(there != me)
            def _(there=there):
                act(scatter(u, there))

    def step(u, carry):
        product = lax.dot_general(
            mat_ref[pl.ds(pl.multiple_of(u * stride, stride), stride)],
            fields_ref[...], (((1,), (1,)), ((), ())), preferred_element_type=jnp.float32,
        )
        turned = product.T
        summed = turned[:columns] + turned[columns:]
        for part in range(parts):
            out_buf[u, :, part, 0, :] = summed[:, part * LANES : (part + 1) * LANES]
        each_target(u, lambda copy: copy.start())
        return carry

    lax.fori_loop(0, steps, step, 0)
    forward(1)
    images_of(group)

    first_turn = (me // nb) * turns
    mine = pl.ds(lax.rem(me, nb) * BASIS, BASIS)
    for turn in range(turns):
        in_buf[me, :, pl.ds(turn * parts, parts)] = out_buf[first_turn + turn, mine]
    for t in range(1, n):
        for turn in range(turns):
            gathered(lax.rem(me + t, n), turn).wait_recv()
    for k in range(BASIS):
        summed = in_buf[0, k]
        for source in range(1, n):
            summed = summed + in_buf[source, k]
        total_ref[k] = summed.reshape(total_ref.shape[1:])
    lane = lax.broadcasted_iota(jnp.int32, total_ref.shape[1:], 1)
    gram = jnp.zeros(total_ref.shape[1:], jnp.float32)
    for p, (i, k) in enumerate(PAIRS):
        value = jnp.sum(total_ref[i] * total_ref[k], axis=1, keepdims=True)
        gram = jnp.where(lane == p, value, gram)
    own = group * n + me
    gram_all[own] = jnp.sum(gram, axis=0, keepdims=True)

    def share(dz, dd):
        return remote(
            gram_all.at[own], gram_all.at[own], g_send.at[dz * n + dd], g_recv.at[own],
            dom=lax.rem(me + dd, n), shift=lax.rem(group + dz, groups),
        )

    def shared(t):
        slot = lax.rem(own + t, groups * n)
        return remote(
            gram_all.at[slot], gram_all.at[slot], g_send.at[t], g_recv.at[slot],
            dom=right, shift=group,
        )

    def every(act):
        def one(t, carry):
            act(share(t // n, lax.rem(t, n)))
            return carry

        lax.fori_loop(1, groups * n, one, 0)

    every(lambda copy: copy.start())
    for i in range(2, groups):
        forward(i)
    for i in range(1, groups):
        settled(i)
        images_of(other(i))

    def wait_shared(t, carry):
        shared(t).wait_recv()
        return carry

    lax.fori_loop(1, groups * n, wait_shared, 0)
    for t in range(groups * n):
        gram_rows[t : t + 1] = gram_all[t]
    tau = jnp.zeros((1, LANES), jnp.float32)
    lane_row = lax.broadcasted_iota(jnp.int32, (1, LANES), 1)
    for j in range(shifts):
        tau = jnp.where(lane_row == j, table_ref[ids_ref[j]] - MID, tau)
    count = groups * nb
    grams = gram_rows[...]
    if n > nb:
        grams = jnp.sum(grams.reshape(groups, n // nb, nb, LANES), axis=1).reshape(count, LANES)
    for q, value in enumerate(weights(coefficients(grams, tau), tau)):
        for j in range(shifts):
            c_ref[q * shifts + j] = jnp.broadcast_to(value[:, j : j + 1], (count, LANES))

    @pl.when(has_right)
    def _():
        halo(group, 0).wait_send()
        for i in range(1, groups):
            halo(other(i), 0).wait_send()
        for which in range(2):
            coeff_halo(which, 0).wait_send()

    @pl.when(has_left)
    def _():
        halo(group, 1).wait_send()
        for i in range(1, groups):
            halo(other(i), 1).wait_send()
        for which in range(2):
            coeff_halo(which, 1).wait_send()

    for i in range(groups):
        slot = other(i)

        @pl.when(up_from(slot))
        def _():
            across(slot, 0).wait_send()

        @pl.when(down_from(slot))
        def _():
            across(slot, 1).wait_send()

    def sent(u, carry):
        each_target(u, lambda copy: copy.wait_send())
        return carry

    lax.fori_loop(0, steps, sent, 0)
    every(lambda copy: copy.wait_send())


def combine_kernel(image_ref, c_ref, sol_ref, res_ref):
    shifts, batch = sol_ref.shape[0], sol_ref.shape[1]
    first = pl.program_id(0) * batch

    def one_source(i, carry):
        b = first + i
        w0 = image_ref[0, b]
        for j in range(shifts):
            z0 = image_ref[1 + j, b]
            z1 = image_ref[1 + shifts + j, b]
            z2 = image_ref[1 + 2 * shifts + j, b]
            of_w0, of_z0, of_z1, c0, c1, c2 = [
                c_ref[q * shifts + j, pl.ds(b, 1)] for q in range(WEIGHTS)
            ]
            sol_ref[j, i] = of_w0 * w0 + of_z0 * z0 + of_z1 * z1
            res_ref[j, i] = w0 - c0 * z0 - c1 * z1 - c2 * z2
        return carry

    lax.fori_loop(0, batch, one_source, 0)


def on_device(sources, kappa, mass, shift_table, shift_ids, sketch):
    n, groups = lax.axis_size("dom"), lax.axis_size("shift")
    nb, slab = sources.shape[0], sources.shape[1]
    tail = sources.shape[2:]
    shifts = shift_ids.shape[0]
    rows = sketch.shape[0]
    block = rows // 8
    cells = slab * tail[0] * tail[1]
    planes = slab + 2 * HALO
    count = groups * nb
    columns = BASIS * nb
    stride = rows // STEPS
    parts = stride // LANES
    chunk = rows // (n // nb)
    turns = chunk // stride
    vmem = pl.BlockSpec(memory_space=pltpu.VMEM)
    hbm = pl.BlockSpec(memory_space=pl.ANY)
    smem = pl.BlockSpec(memory_space=pltpu.SMEM)
    dma = pltpu.SemaphoreType.DMA
    f32 = jnp.float32
    images, solved = pl.pallas_call(
        functools.partial(project_kernel, n, groups),
        out_shape=(
            pltpu.VMEM((1 + 3 * shifts, count, slab) + tail, f32),
            pltpu.VMEM((WEIGHTS * shifts, count, LANES), f32),
        ),
        in_specs=[hbm, hbm, hbm, smem, smem, hbm],
        out_specs=(vmem, vmem),
        scratch_shapes=[
            pltpu.VMEM((groups, nb, planes) + tail, f32),
            pltpu.VMEM((2, planes) + tail, f32),
            pltpu.VMEM((rows // block, block, slab) + tail, jnp.bfloat16),
            pltpu.VMEM((rows, cells), jnp.bfloat16),
            pltpu.VMEM((2 * columns, slab) + tail, jnp.bfloat16),
            pltpu.VMEM((2 * columns, cells), jnp.bfloat16),
            pltpu.VMEM((STEPS, columns, parts, 1, LANES), f32),
            pltpu.VMEM((n, BASIS, turns * parts, 1, LANES), f32),
            pltpu.VMEM((BASIS, turns * parts, LANES), f32),
            pltpu.VMEM((groups * n, 1, LANES), f32),
            pltpu.VMEM((groups * n, LANES), f32),
            dma((rows // block,)), dma((3,)),
            dma((groups, 2)), dma((groups,)),
            dma((groups, 2)), dma((groups, 2)),
            dma((2, 2)), dma((2, 2)),
            dma((STEPS, nb)), dma((n, turns)),
            dma((groups * n,)), dma((groups * n,)),
        ],
        compiler_params=pltpu.CompilerParams(
            collective_id=0, has_side_effects=True, vmem_limit_bytes=46 << 20
        ),
        name="project",
    )(sources, kappa, mass, shift_table, shift_ids, sketch)

    batch = 4 if count % 4 == 0 else 1
    out = jax.ShapeDtypeStruct((shifts, count, slab) + tail, f32)
    out_spec = pl.BlockSpec((shifts, batch, slab) + tail, lambda i: (0, i, 0, 0, 0))
    return pl.pallas_call(
        combine_kernel,
        grid=(count // batch,),
        out_shape=(out, out),
        in_specs=[vmem, vmem],
        out_specs=(out_spec, out_spec),
        compiler_params=pltpu.CompilerParams(vmem_limit_bytes=32 << 20),
        name="combine",
    )(
        pltpu.with_memory_space_constraint(images, pltpu.VMEM),
        pltpu.with_memory_space_constraint(solved, pltpu.VMEM),
    )


def solution(mesh):
    placed = (
        P("shift", "dom", None, None),
        P("dom", None, None),
        P("dom", None, None),
        P(),
        P("shift"),
        P(None, "dom", None, None),
    )
    return jax.shard_map(
        on_device,
        mesh=mesh,
        in_specs=placed,
        out_specs=(P("shift", None, "dom", None, None), P("shift", None, "dom", None, None)),
        check_vma=False,
    )
```

```python
import functools

import jax
import jax.numpy as jnp
from jax import lax
from jax.experimental import pallas as pl
from jax.experimental.pallas import tpu as pltpu
from jax.sharding import PartitionSpec as P

HALO = 3
STEPS = 4
HALVES = 2
EARLY = 3
LANES = 128
MID = 2.25
BASIS = 10
WEIGHTS = 6
IMAGES = ((1, 2), (3, 4, 5), (6, 7, 8, 9))
PAIRS = [(i, k) for i in range(BASIS) for k in range(i, BASIS)]
PAIR_INDEX = {pair: n for n, pair in enumerate(PAIRS)}


def neighbour_sum(field):
    inner = field[1:-1]
    shape = inner.shape
    total = field[2:] + field[:-2]
    for dim in (1, 2):
        size = shape[dim]
        place = lax.broadcasted_iota(jnp.int32, shape, dim)
        total = total + jnp.where(place > 0, pltpu.roll(inner, 1, dim), 0.0)
        total = total + jnp.where(place < size - 1, pltpu.roll(inner, size - 1, dim), 0.0)
    return total


def plane_mask(shape, width, low, high):
    plane = lax.broadcasted_iota(jnp.int32, shape, 0)
    return jnp.where(plane < width, low, jnp.where(plane >= shape[0] - width, high, 1.0))


def edge_flags():
    me = lax.axis_index("dom")
    last = lax.axis_size("dom") - 1
    return (me > 0).astype(jnp.float32), (me < last).astype(jnp.float32)


def basis_fields(w0, diag, mass, mask1, mask2):
    sixth = 1.0 / 6.0
    center = 6.0 + MID
    d1, m1 = diag[1:-1], mass[1:-1]
    d2, m2 = diag[2:-2], mass[2:-2]
    d3, m3 = diag[3:-3], mass[3:-3]
    w0i = w0[1:-1]
    a0 = d1 * w0i - neighbour_sum(w0)
    a1 = m1 * w0i
    scaled1 = sixth * mask1
    g0 = (a0 - center * w0i) * scaled1
    g1 = (a1 - w0i) * scaled1
    g0i, g1i = g0[1:-1], g1[1:-1]
    b0 = d2 * g0i - neighbour_sum(g0)
    b1 = d2 * g1i - neighbour_sum(g1) + m2 * g0i
    b2 = m2 * g1i
    scaled2 = sixth * mask2
    h0 = (b0 - center * g0i) * scaled2
    h1 = (b1 - center * g1i - g0i) * scaled2
    h2 = (b2 - g1i) * scaled2
    h0i, h1i, h2i = h0[1:-1], h1[1:-1], h2[1:-1]
    e0 = d3 * h0i - neighbour_sum(h0)
    e1 = d3 * h1i - neighbour_sum(h1) + m3 * h0i
    e2 = d3 * h2i - neighbour_sum(h2) + m3 * h1i
    e3 = m3 * h2i
    return [
        w0[3:-3], a0[2:-2], a1[2:-2], b0[1:-1], b1[1:-1], b2[1:-1], e0, e1, e2, e3
    ]


def solve_small(h_vals, entry):
    l00 = jnp.sqrt(entry[0][0])
    l10 = entry[1][0] / l00
    l20 = entry[2][0] / l00
    l11 = jnp.sqrt(entry[1][1] - l10 * l10)
    l21 = (entry[2][1] - l20 * l10) / l11
    l22 = jnp.sqrt(entry[2][2] - l20 * l20 - l21 * l21)
    f0 = h_vals[0] / l00
    f1 = (h_vals[1] - l10 * f0) / l11
    f2 = (h_vals[2] - l20 * f0 - l21 * f1) / l22
    c2 = f2 / l22
    c1 = (f1 - l21 * c2) / l11
    c0 = (f0 - l10 * c1 - l20 * c2) / l00
    return (c0, c1, c2)


def coefficients(gram, tau):
    def product(left, right):
        by_degree = {}
        for p, i in enumerate(left):
            for q, k in enumerate(right):
                n = PAIR_INDEX[(min(i, k), max(i, k))]
                column = gram[:, n : n + 1]
                by_degree[p + q] = by_degree[p + q] + column if p + q in by_degree else column
        top = max(by_degree)
        total = jnp.broadcast_to(by_degree[top], (gram.shape[0], LANES))
        for degree in range(top - 1, -1, -1):
            total = total * tau + by_degree[degree]
        return total

    h_vals = [product(image, (0,)) for image in IMAGES]
    entry = [[None] * 3 for _ in range(3)]
    for i in range(3):
        for k in range(i + 1):
            entry[i][k] = product(IMAGES[i], IMAGES[k])
    ridge = 0.001 * (entry[0][0] + entry[1][1] + entry[2][2]) / 3.0 + 1.0
    for i in range(3):
        entry[i][i] = entry[i][i] + ridge
    return solve_small(h_vals, entry)


def weights(solved, tau):
    c0, c1, c2 = solved
    shifted = 6.0 + MID + tau
    of_z1 = c2 * (1.0 / 6.0)
    of_z0 = (c1 - of_z1 * shifted) * (1.0 / 6.0)
    of_w0 = c0 - of_z0 * shifted
    return (of_w0, of_z0, of_z1, c0, c1, c2)


def project_kernel(
    n, groups, src_hbm, kappa_hbm, mass_hbm, table_ref, ids_ref, sketch_ref,
    image_ref, c_ref,
    wide_ref, coeff_ref, rows_buf, mat_ref, raw_ref, fields_ref, out_buf, in_buf, total_ref, gram_all,
    gram_rows, load_sem, in_sem, z_send, z_recv, halo_send, halo_recv, km_send, km_recv,
    rs_send, rs_recv, g_send, g_recv,
):
    me = lax.axis_index("dom")
    group = lax.axis_index("shift")
    nb = wide_ref.shape[1]
    slab = wide_ref.shape[2] - 2 * HALO
    tail = wide_ref.shape[3:]
    shifts = ids_ref.shape[0]
    columns = BASIS * nb
    rows = mat_ref.shape[0]
    blocks, block = rows_buf.shape[0], rows_buf.shape[1]
    steps = out_buf.shape[0]
    stride = rows // steps
    parts = stride // LANES
    chunk = rows // (n // nb)
    turns = chunk // stride
    right, left = lax.rem(me + 1, n), lax.rem(me + n - 1, n)
    has_right, has_left = me < n - 1, me > 0
    has_up, has_down = group < groups - 1, group > 0
    upper = (2 * group) // groups
    nearer = group + upper * (groups - 1 - 2 * group)

    def remote(src, dst, send, recv, **where):
        return pltpu.make_async_remote_copy(
            src_ref=src, dst_ref=dst, send_sem=send, recv_sem=recv,
            device_id=where, device_id_type=pl.DeviceIdType.MESH,
        )

    def load(t):
        return pltpu.make_async_copy(
            sketch_ref.at[pl.ds(t * block, block)], rows_buf.at[t], load_sem.at[t]
        )

    barrier = pltpu.get_barrier_semaphore()
    for t in range(1, n):
        pl.semaphore_signal(
            barrier, inc=1, device_id={"dom": lax.rem(me + t, n)},
            device_id_type=pl.DeviceIdType.MESH,
        )
    for t in range(1, groups):
        pl.semaphore_signal(
            barrier, inc=1, device_id={"shift": lax.rem(group + t, groups)},
            device_id_type=pl.DeviceIdType.MESH,
        )
    inner = pl.ds(HALO, slab)
    arguments = [
        pltpu.make_async_copy(src_hbm, wide_ref.at[group, :, inner], in_sem.at[0]),
        pltpu.make_async_copy(kappa_hbm, coeff_ref.at[0, inner], in_sem.at[1]),
        pltpu.make_async_copy(mass_hbm, coeff_ref.at[1, inner], in_sem.at[2]),
    ]
    for copy in arguments:
        copy.start()
    for t in range(blocks):
        load(t).start()

    @pl.when(jnp.logical_not(has_left))
    def _():
        wide_ref[:, :, pl.ds(0, HALO)] = jnp.zeros((groups, nb, HALO) + tail, jnp.float32)
        coeff_ref[:, pl.ds(0, HALO)] = jnp.zeros((2, HALO) + tail, jnp.float32)

    @pl.when(jnp.logical_not(has_right))
    def _():
        wide_ref[:, :, pl.ds(slab + HALO, HALO)] = jnp.zeros(
            (groups, nb, HALO) + tail, jnp.float32
        )
        coeff_ref[:, pl.ds(slab + HALO, HALO)] = jnp.zeros((2, HALO) + tail, jnp.float32)

    def settle(t, carry):
        load(t).wait()
        mat_ref[pl.ds(pl.multiple_of(t * block, block), block)] = rows_buf[t].reshape(
            block, mat_ref.shape[1]
        )
        return carry

    lax.fori_loop(0, EARLY, settle, 0)
    for copy in arguments:
        copy.wait()
    pl.semaphore_wait(barrier, n - 1 + groups - 1)

    def sides(side):
        if side == 0:
            return pl.ds(slab, HALO), pl.ds(0, HALO), right
        return pl.ds(HALO, HALO), pl.ds(slab + HALO, HALO), left

    def halo(slot, side, part):
        first, target, there = sides(side)
        some = pl.ds(part * (nb // HALVES), nb // HALVES)
        return remote(
            wide_ref.at[slot, some, first], wide_ref.at[slot, some, target],
            halo_send.at[slot, side, part], halo_recv.at[slot, side, part], dom=there,
        )

    def coeff_halo(which, side):
        first, target, there = sides(side)
        return remote(
            coeff_ref.at[which, first], coeff_ref.at[which, target], km_send.at[which, side],
            km_recv.at[which, side], dom=there,
        )

    def across(slot, way):
        return remote(
            wide_ref.at[slot, :, inner], wide_ref.at[slot, :, inner],
            z_send.at[slot, way], z_recv.at[slot],
            shift=group + 1 - 2 * way,
        )

    def other(i):
        if i == 0:
            return group
        longer = 1 - 2 * upper
        both = (2 * nearer - i + groups) // groups
        swing = longer * ((i + 1) // 2) * (1 if i % 2 else -1)
        return group + both * swing + (1 - both) * longer * (i - nearer)

    def to_right(act):
        pl.when(has_right)(act)

    def to_left(act):
        pl.when(has_left)(act)

    def up_from(slot):
        return jnp.logical_and(slot <= group, has_up)

    def down_from(slot):
        return jnp.logical_and(slot >= group, has_down)

    @pl.when(has_right)
    def _():
        for part in range(HALVES):
            halo(group, 0, part).start()
        for which in range(2):
            coeff_halo(which, 0).start()

    @pl.when(has_left)
    def _():
        for part in range(HALVES):
            halo(group, 1, part).start()
        for which in range(2):
            coeff_halo(which, 1).start()

    @pl.when(has_up)
    def _():
        across(group, 0).start()

    @pl.when(has_down)
    def _():
        across(group, 1).start()

    lax.fori_loop(EARLY, blocks, settle, 0)

    @pl.when(has_left)
    def _():
        for part in range(HALVES):
            halo(group, 0, part).wait_recv()
        for which in range(2):
            coeff_halo(which, 0).wait_recv()

    @pl.when(has_right)
    def _():
        for part in range(HALVES):
            halo(group, 1, part).wait_recv()
        for which in range(2):
            coeff_halo(which, 1).wait_recv()

    half = nb // HALVES

    def relayed(slot):
        below = jnp.logical_and(slot < group, has_up)
        return jnp.logical_or(below, jnp.logical_and(slot > group, has_down))

    def pass_on(i):
        slot = other(i)

        @pl.when(relayed(slot))
        def _():
            across(slot, 0).wait_recv()

        @pl.when(up_from(slot))
        def _():
            across(slot, 0).start()

        @pl.when(down_from(slot))
        def _():
            across(slot, 1).start()

    def spread_planes(i):
        slot = other(i)

        @pl.when(jnp.logical_not(relayed(slot)))
        def _():
            across(slot, 0).wait_recv()

        for part in range(HALVES):
            @pl.when(has_right)
            def _():
                halo(slot, 0, part).start()

            @pl.when(has_left)
            def _():
                halo(slot, 1, part).start()

    def settled(slot, part):
        @pl.when(has_left)
        def _():
            halo(slot, 0, part).wait_recv()

        @pl.when(has_right)
        def _():
            halo(slot, 1, part).wait_recv()

    for i in range(1, min(groups, 3)):
        pass_on(i)
    spread_planes(1)
    low, high = edge_flags()
    planes = slab + 2 * HALO

    def basis_of(slot, b):
        mass = coeff_ref[1]
        diag = (6.0 - coeff_ref[0]) + MID * mass
        mask1 = plane_mask((planes - 2,) + tail, 2, low, high)
        mask2 = plane_mask((planes - 4,) + tail, 1, low, high)
        return basis_fields(wide_ref[slot, b], diag, mass, mask1, mask2)

    def one_source(b, carry):
        for k, field in enumerate(basis_of(group, b)):
            rounded = field.astype(jnp.bfloat16)
            raw_ref[b * BASIS + k] = rounded
            raw_ref[columns + b * BASIS + k] = (field - rounded.astype(jnp.float32)).astype(
                jnp.bfloat16
            )
        return carry

    lax.fori_loop(0, nb, one_source, 0)
    fields_ref[...] = raw_ref[...].reshape(fields_ref.shape)

    def images_of(slot, part):
        def one(b, carry):
            w0, a0, a1, b0, b1, b2, e0, e1, e2, e3 = basis_of(slot, b)
            place = slot * nb + b
            image_ref[0, place] = w0
            for j in range(shifts):
                tau = table_ref[ids_ref[j]] - MID
                image_ref[1 + j, place] = a0 + tau * a1
                image_ref[1 + shifts + j, place] = b0 + tau * (b1 + tau * b2)
                image_ref[1 + 2 * shifts + j, place] = e0 + tau * (e1 + tau * (e2 + tau * e3))
            return carry

        lax.fori_loop(part * half, (part + 1) * half, one, 0)

    def scatter(u, there):
        turn = lax.rem(u, turns)
        return remote(
            out_buf.at[u, pl.ds(lax.rem(there, nb) * BASIS, BASIS)],
            in_buf.at[me, :, pl.ds(turn * parts, parts)],
            rs_send.at[u, lax.rem(there, nb)], rs_recv, dom=there,
        )

    def each_target(u, act):
        base = (u // turns) * nb
        for t in range(1, nb + 1):
            there = base + lax.rem(me + t, nb)

            @pl.when(there != me)
            def _(there=there):
                act(scatter(u, there))

    def step(u, carry):
        product = lax.dot_general(
            mat_ref[pl.ds(pl.multiple_of(u * stride, stride), stride)],
            fields_ref[...], (((1,), (1,)), ((), ())), preferred_element_type=jnp.float32,
        )
        turned = product.T
        summed = turned[:columns] + turned[columns:]
        for part in range(parts):
            out_buf[u, :, part, 0, :] = summed[:, part * LANES : (part + 1) * LANES]
        each_target(u, lambda copy: copy.start())
        return carry

    lax.fori_loop(0, steps // 2, step, 0)
    for i in range(3, groups):
        pass_on(i)
    lax.fori_loop(steps // 2, steps, step, 0)
    spread_planes(2)
    for part in range(HALVES):
        images_of(group, part)
    for part in range(HALVES):
        settled(other(1), part)
        images_of(other(1), part)

    first_turn = (me // nb) * turns
    mine = pl.ds(lax.rem(me, nb) * BASIS, BASIS)
    for turn in range(turns):
        in_buf[me, :, pl.ds(turn * parts, parts)] = out_buf[first_turn + turn, mine]
    remote(
        in_buf.at[pl.ds(0, n - 1)], in_buf.at[pl.ds(0, n - 1)], rs_send.at[0, 0], rs_recv, dom=right
    ).wait_recv()
    for k in range(BASIS):
        summed = in_buf[0, k]
        for source in range(1, n):
            summed = summed + in_buf[source, k]
        total_ref[k] = summed.reshape(total_ref.shape[1:])
    lane = lax.broadcasted_iota(jnp.int32, total_ref.shape[1:], 1)
    gram = jnp.zeros(total_ref.shape[1:], jnp.float32)
    for p, (i, k) in enumerate(PAIRS):
        value = jnp.sum(total_ref[i] * total_ref[k], axis=1, keepdims=True)
        gram = jnp.where(lane == p, value, gram)
    own = group * n + me
    gram_all[own] = jnp.sum(gram, axis=0, keepdims=True)

    def every(act):
        for dz in range(groups - 1, -1, -1):
            there = lax.rem(group + dz, groups)
            for dd in range(n):
                if dz or dd:
                    act(there, lax.rem(me + dd, n))

    def share(there, where):
        remote(
            gram_all.at[own], gram_all.at[own], g_send, g_recv, dom=where, shift=there
        ).start()

    others = gram_all.at[pl.ds(0, groups * n - 1)]
    everybody = remote(others, others, g_send, g_recv, dom=right)
    every(share)
    for i in range(3, groups):
        spread_planes(i)
    for i in range(2, groups):
        for part in range(HALVES):
            settled(other(i), part)
            images_of(other(i), part)

    everybody.wait_recv()
    for t in range(groups * n):
        gram_rows[t : t + 1] = gram_all[t]
    tau = jnp.zeros((1, LANES), jnp.float32)
    lane_row = lax.broadcasted_iota(jnp.int32, (1, LANES), 1)
    for j in range(shifts):
        tau = jnp.where(lane_row == j, table_ref[ids_ref[j]] - MID, tau)
    count = groups * nb
    grams = gram_rows[...]
    if n > nb:
        grams = jnp.sum(grams.reshape(groups, n // nb, nb, LANES), axis=1).reshape(count, LANES)
    for q, value in enumerate(weights(coefficients(grams, tau), tau)):
        for j in range(shifts):
            c_ref[q * shifts + j] = jnp.broadcast_to(value[:, j : j + 1], (count, LANES))

    @pl.when(has_right)
    def _():
        for i in range(groups):
            for part in range(HALVES):
                halo(other(i), 0, part).wait_send()
        for which in range(2):
            coeff_halo(which, 0).wait_send()

    @pl.when(has_left)
    def _():
        for i in range(groups):
            for part in range(HALVES):
                halo(other(i), 1, part).wait_send()
        for which in range(2):
            coeff_halo(which, 1).wait_send()

    for i in range(groups):
        slot = other(i)

        @pl.when(up_from(slot))
        def _():
            across(slot, 0).wait_send()

        @pl.when(down_from(slot))
        def _():
            across(slot, 1).wait_send()

    def sent(u, carry):
        each_target(u, lambda copy: copy.wait_send())
        return carry

    lax.fori_loop(0, steps, sent, 0)
    everybody.wait_send()


def combine_kernel(image_ref, c_ref, sol_ref, res_ref):
    shifts, batch = sol_ref.shape[0], sol_ref.shape[1]
    first = pl.program_id(0) * batch

    def one_source(i, carry):
        b = first + i
        w0 = image_ref[0, b]
        for j in range(shifts):
            z0 = image_ref[1 + j, b]
            z1 = image_ref[1 + shifts + j, b]
            z2 = image_ref[1 + 2 * shifts + j, b]
            of_w0, of_z0, of_z1, c0, c1, c2 = [
                c_ref[q * shifts + j, pl.ds(b, 1)] for q in range(WEIGHTS)
            ]
            sol_ref[j, i] = of_w0 * w0 + of_z0 * z0 + of_z1 * z1
            res_ref[j, i] = w0 - c0 * z0 - c1 * z1 - c2 * z2
        return carry

    lax.fori_loop(0, batch, one_source, 0)


def on_device(sources, kappa, mass, shift_table, shift_ids, sketch):
    n, groups = lax.axis_size("dom"), lax.axis_size("shift")
    nb, slab = sources.shape[0], sources.shape[1]
    tail = sources.shape[2:]
    shifts = shift_ids.shape[0]
    rows = sketch.shape[0]
    block = rows // 8
    cells = slab * tail[0] * tail[1]
    planes = slab + 2 * HALO
    count = groups * nb
    columns = BASIS * nb
    stride = rows // STEPS
    parts = stride // LANES
    chunk = rows // (n // nb)
    turns = chunk // stride
    vmem = pl.BlockSpec(memory_space=pltpu.VMEM)
    hbm = pl.BlockSpec(memory_space=pl.ANY)
    smem = pl.BlockSpec(memory_space=pltpu.SMEM)
    dma = pltpu.SemaphoreType.DMA
    f32 = jnp.float32
    images, solved = pl.pallas_call(
        functools.partial(project_kernel, n, groups),
        out_shape=(
            pltpu.VMEM((1 + 3 * shifts, count, slab) + tail, f32),
            pltpu.VMEM((WEIGHTS * shifts, count, LANES), f32),
        ),
        in_specs=[hbm, hbm, hbm, smem, smem, hbm],
        out_specs=(vmem, vmem),
        scratch_shapes=[
            pltpu.VMEM((groups, nb, planes) + tail, f32),
            pltpu.VMEM((2, planes) + tail, f32),
            pltpu.VMEM((rows // block, block, slab) + tail, jnp.bfloat16),
            pltpu.VMEM((rows, cells), jnp.bfloat16),
            pltpu.VMEM((2 * columns, slab) + tail, jnp.bfloat16),
            pltpu.VMEM((2 * columns, cells), jnp.bfloat16),
            pltpu.VMEM((STEPS, columns, parts, 1, LANES), f32),
            pltpu.VMEM((n, BASIS, turns * parts, 1, LANES), f32),
            pltpu.VMEM((BASIS, turns * parts, LANES), f32),
            pltpu.VMEM((groups * n, 1, LANES), f32),
            pltpu.VMEM((groups * n, LANES), f32),
            dma((rows // block,)), dma((3,)),
            dma((groups, 2)), dma((groups,)),
            dma((groups, 2, HALVES)), dma((groups, 2, HALVES)),
            dma((2, 2)), dma((2, 2)),
            dma((STEPS, nb)), dma,
            dma, dma,
        ],
        compiler_params=pltpu.CompilerParams(
            collective_id=0, has_side_effects=True, vmem_limit_bytes=46 << 20
        ),
        name="project",
    )(sources, kappa, mass, shift_table, shift_ids, sketch)

    batch = 4 if count % 4 == 0 else 1
    out = jax.ShapeDtypeStruct((shifts, count, slab) + tail, f32)
    out_spec = pl.BlockSpec((shifts, batch, slab) + tail, lambda i: (0, i, 0, 0, 0))
    return pl.pallas_call(
        combine_kernel,
        grid=(count // batch,),
        out_shape=(out, out),
        in_specs=[vmem, vmem],
        out_specs=(out_spec, out_spec),
        compiler_params=pltpu.CompilerParams(vmem_limit_bytes=32 << 20),
        name="combine",
    )(
        pltpu.with_memory_space_constraint(images, pltpu.VMEM),
        pltpu.with_memory_space_constraint(solved, pltpu.VMEM),
    )


def solution(mesh):
    placed = (
        P("shift", "dom", None, None),
        P("dom", None, None),
        P("dom", None, None),
        P(),
        P("shift"),
        P(None, "dom", None, None),
    )
    return jax.shard_map(
        on_device,
        mesh=mesh,
        in_specs=placed,
        out_specs=(P("shift", None, "dom", None, None), P("shift", None, "dom", None, None)),
        check_vma=False,
    )
```

```python
import functools

import jax
import jax.numpy as jnp
from jax import lax
from jax.experimental import pallas as pl
from jax.experimental.pallas import tpu as pltpu
from jax.sharding import PartitionSpec as P

HALO = 3
STEPS = 4
HALVES = 2
EARLY = 3
LANES = 128
MID = 2.25
BASIS = 10
WEIGHTS = 6
IMAGES = ((1, 2), (3, 4, 5), (6, 7, 8, 9))
PAIRS = [(i, k) for i in range(BASIS) for k in range(i, BASIS)]
PAIR_INDEX = {pair: n for n, pair in enumerate(PAIRS)}


def neighbour_sum(field):
    inner = field[1:-1]
    shape = inner.shape
    total = field[2:] + field[:-2]
    for dim in (1, 2):
        size = shape[dim]
        place = lax.broadcasted_iota(jnp.int32, shape, dim)
        total = total + jnp.where(place > 0, pltpu.roll(inner, 1, dim), 0.0)
        total = total + jnp.where(place < size - 1, pltpu.roll(inner, size - 1, dim), 0.0)
    return total


def plane_mask(shape, width, low, high):
    plane = lax.broadcasted_iota(jnp.int32, shape, 0)
    return jnp.where(plane < width, low, jnp.where(plane >= shape[0] - width, high, 1.0))


def edge_flags():
    me = lax.axis_index("dom")
    last = lax.axis_size("dom") - 1
    return (me > 0).astype(jnp.float32), (me < last).astype(jnp.float32)


def basis_fields(w0, diag, mass, mask1, mask2):
    sixth = 1.0 / 6.0
    center = 6.0 + MID
    d1, m1 = diag[1:-1], mass[1:-1]
    d2, m2 = diag[2:-2], mass[2:-2]
    d3, m3 = diag[3:-3], mass[3:-3]
    w0i = w0[1:-1]
    a0 = d1 * w0i - neighbour_sum(w0)
    a1 = m1 * w0i
    scaled1 = sixth * mask1
    g0 = (a0 - center * w0i) * scaled1
    g1 = (a1 - w0i) * scaled1
    g0i, g1i = g0[1:-1], g1[1:-1]
    b0 = d2 * g0i - neighbour_sum(g0)
    b1 = d2 * g1i - neighbour_sum(g1) + m2 * g0i
    b2 = m2 * g1i
    scaled2 = sixth * mask2
    h0 = (b0 - center * g0i) * scaled2
    h1 = (b1 - center * g1i - g0i) * scaled2
    h2 = (b2 - g1i) * scaled2
    h0i, h1i, h2i = h0[1:-1], h1[1:-1], h2[1:-1]
    e0 = d3 * h0i - neighbour_sum(h0)
    e1 = d3 * h1i - neighbour_sum(h1) + m3 * h0i
    e2 = d3 * h2i - neighbour_sum(h2) + m3 * h1i
    e3 = m3 * h2i
    return [
        w0[3:-3], a0[2:-2], a1[2:-2], b0[1:-1], b1[1:-1], b2[1:-1], e0, e1, e2, e3
    ]


def solve_small(h_vals, entry):
    l00 = jnp.sqrt(entry[0][0])
    l10 = entry[1][0] / l00
    l20 = entry[2][0] / l00
    l11 = jnp.sqrt(entry[1][1] - l10 * l10)
    l21 = (entry[2][1] - l20 * l10) / l11
    l22 = jnp.sqrt(entry[2][2] - l20 * l20 - l21 * l21)
    f0 = h_vals[0] / l00
    f1 = (h_vals[1] - l10 * f0) / l11
    f2 = (h_vals[2] - l20 * f0 - l21 * f1) / l22
    c2 = f2 / l22
    c1 = (f1 - l21 * c2) / l11
    c0 = (f0 - l10 * c1 - l20 * c2) / l00
    return (c0, c1, c2)


def coefficients(gram, tau):
    def product(left, right):
        by_degree = {}
        for p, i in enumerate(left):
            for q, k in enumerate(right):
                n = PAIR_INDEX[(min(i, k), max(i, k))]
                column = gram[:, n : n + 1]
                by_degree[p + q] = by_degree[p + q] + column if p + q in by_degree else column
        top = max(by_degree)
        total = jnp.broadcast_to(by_degree[top], (gram.shape[0], LANES))
        for degree in range(top - 1, -1, -1):
            total = total * tau + by_degree[degree]
        return total

    h_vals = [product(image, (0,)) for image in IMAGES]
    entry = [[None] * 3 for _ in range(3)]
    for i in range(3):
        for k in range(i + 1):
            entry[i][k] = product(IMAGES[i], IMAGES[k])
    ridge = 0.001 * (entry[0][0] + entry[1][1] + entry[2][2]) / 3.0 + 1.0
    for i in range(3):
        entry[i][i] = entry[i][i] + ridge
    return solve_small(h_vals, entry)


def weights(solved, tau):
    c0, c1, c2 = solved
    shifted = 6.0 + MID + tau
    of_z1 = c2 * (1.0 / 6.0)
    of_z0 = (c1 - of_z1 * shifted) * (1.0 / 6.0)
    of_w0 = c0 - of_z0 * shifted
    return (of_w0, of_z0, of_z1, c0, c1, c2)


def project_kernel(
    n, groups, src_hbm, kappa_hbm, mass_hbm, table_ref, ids_ref, sketch_ref,
    image_ref, c_ref,
    wide_ref, coeff_ref, rows_buf, mat_ref, raw_ref, fields_ref, out_buf, in_buf, total_ref, gram_all,
    gram_rows, load_sem, in_sem, z_send, z_recv, halo_send, halo_recv, km_send, km_recv,
    rs_send, rs_recv, g_send, g_recv,
):
    me = lax.axis_index("dom")
    group = lax.axis_index("shift")
    nb = wide_ref.shape[1]
    slab = wide_ref.shape[2] - 2 * HALO
    tail = wide_ref.shape[3:]
    shifts = ids_ref.shape[0]
    columns = BASIS * nb
    rows = mat_ref.shape[0]
    blocks, block = rows_buf.shape[0], rows_buf.shape[1]
    steps = out_buf.shape[0]
    stride = rows // steps
    parts = stride // LANES
    chunk = rows // (n // nb)
    turns = chunk // stride
    right, left = lax.rem(me + 1, n), lax.rem(me + n - 1, n)
    has_right, has_left = me < n - 1, me > 0
    has_up, has_down = group < groups - 1, group > 0
    upper = (2 * group) // groups
    nearer = group + upper * (groups - 1 - 2 * group)

    def remote(src, dst, send, recv, **where):
        return pltpu.make_async_remote_copy(
            src_ref=src, dst_ref=dst, send_sem=send, recv_sem=recv,
            device_id=where, device_id_type=pl.DeviceIdType.MESH,
        )

    def load(t):
        return pltpu.make_async_copy(
            sketch_ref.at[pl.ds(t * block, block)], rows_buf.at[t], load_sem.at[t]
        )

    barrier = pltpu.get_barrier_semaphore()
    for t in range(1, n):
        pl.semaphore_signal(
            barrier, inc=1, device_id={"dom": lax.rem(me + t, n)},
            device_id_type=pl.DeviceIdType.MESH,
        )
    for t in range(1, groups):
        pl.semaphore_signal(
            barrier, inc=1, device_id={"shift": lax.rem(group + t, groups)},
            device_id_type=pl.DeviceIdType.MESH,
        )
    inner = pl.ds(HALO, slab)
    arguments = [
        pltpu.make_async_copy(src_hbm, wide_ref.at[group, :, inner], in_sem.at[0]),
        pltpu.make_async_copy(kappa_hbm, coeff_ref.at[0, inner], in_sem.at[1]),
        pltpu.make_async_copy(mass_hbm, coeff_ref.at[1, inner], in_sem.at[2]),
    ]
    for copy in arguments:
        copy.start()
    for t in range(blocks):
        load(t).start()

    @pl.when(jnp.logical_not(has_left))
    def _():
        wide_ref[:, :, pl.ds(0, HALO)] = jnp.zeros((groups, nb, HALO) + tail, jnp.float32)
        coeff_ref[:, pl.ds(0, HALO)] = jnp.zeros((2, HALO) + tail, jnp.float32)

    @pl.when(jnp.logical_not(has_right))
    def _():
        wide_ref[:, :, pl.ds(slab + HALO, HALO)] = jnp.zeros(
            (groups, nb, HALO) + tail, jnp.float32
        )
        coeff_ref[:, pl.ds(slab + HALO, HALO)] = jnp.zeros((2, HALO) + tail, jnp.float32)

    def settle(t, carry):
        load(t).wait()
        mat_ref[pl.ds(pl.multiple_of(t * block, block), block)] = rows_buf[t].reshape(
            block, mat_ref.shape[1]
        )
        return carry

    lax.fori_loop(0, EARLY, settle, 0)
    for copy in arguments:
        copy.wait()
    pl.semaphore_wait(barrier, n - 1 + groups - 1)

    def sides(side):
        if side == 0:
            return pl.ds(slab, HALO), pl.ds(0, HALO), right
        return pl.ds(HALO, HALO), pl.ds(slab + HALO, HALO), left

    def halo(slot, side, part):
        first, target, there = sides(side)
        some = pl.ds(part * (nb // HALVES), nb // HALVES)
        return remote(
            wide_ref.at[slot, some, first], wide_ref.at[slot, some, target],
            halo_send.at[slot, side, part], halo_recv.at[slot, side, part], dom=there,
        )

    def coeff_halo(which, side):
        first, target, there = sides(side)
        return remote(
            coeff_ref.at[which, first], coeff_ref.at[which, target], km_send.at[which, side],
            km_recv.at[which, side], dom=there,
        )

    def across(slot, way, part):
        some = pl.ds(part * (nb // HALVES), nb // HALVES)
        return remote(
            wide_ref.at[slot, some, inner], wide_ref.at[slot, some, inner],
            z_send.at[slot, way, part], z_recv.at[slot, part],
            shift=group + 1 - 2 * way,
        )

    def other(i):
        if i == 0:
            return group
        longer = 1 - 2 * upper
        both = (2 * nearer - i + groups) // groups
        swing = longer * ((i + 1) // 2) * (1 if i % 2 else -1)
        return group + both * swing + (1 - both) * longer * (i - nearer)

    def to_right(act):
        pl.when(has_right)(act)

    def to_left(act):
        pl.when(has_left)(act)

    def up_from(slot):
        return jnp.logical_and(slot <= group, has_up)

    def down_from(slot):
        return jnp.logical_and(slot >= group, has_down)

    @pl.when(has_right)
    def _():
        for which in range(2):
            coeff_halo(which, 0).start()
        for part in range(HALVES):
            halo(group, 0, part).start()

    @pl.when(has_left)
    def _():
        for which in range(2):
            coeff_halo(which, 1).start()
        for part in range(HALVES):
            halo(group, 1, part).start()

    @pl.when(has_up)
    def _():
        for part in range(HALVES):
            across(group, 0, part).start()

    @pl.when(has_down)
    def _():
        for part in range(HALVES):
            across(group, 1, part).start()

    lax.fori_loop(EARLY, blocks, settle, 0)

    @pl.when(has_left)
    def _():
        for which in range(2):
            coeff_halo(which, 0).wait_recv()

    @pl.when(has_right)
    def _():
        for which in range(2):
            coeff_halo(which, 1).wait_recv()

    half = nb // HALVES

    def relayed(slot):
        below = jnp.logical_and(slot < group, has_up)
        return jnp.logical_or(below, jnp.logical_and(slot > group, has_down))

    def pass_on(i):
        slot = other(i)

        for part in range(HALVES):
            @pl.when(relayed(slot))
            def _():
                across(slot, 0, part).wait_recv()

            @pl.when(up_from(slot))
            def _():
                across(slot, 0, part).start()

            @pl.when(down_from(slot))
            def _():
                across(slot, 1, part).start()

    def spread_planes(i):
        slot = other(i)

        for part in range(HALVES):
            @pl.when(jnp.logical_not(relayed(slot)))
            def _():
                across(slot, 0, part).wait_recv()

            @pl.when(has_right)
            def _():
                halo(slot, 0, part).start()

            @pl.when(has_left)
            def _():
                halo(slot, 1, part).start()

    def settled(slot, part):
        @pl.when(has_left)
        def _():
            halo(slot, 0, part).wait_recv()

        @pl.when(has_right)
        def _():
            halo(slot, 1, part).wait_recv()

    low, high = edge_flags()
    planes = slab + 2 * HALO

    def basis_of(slot, b):
        mass = coeff_ref[1]
        diag = (6.0 - coeff_ref[0]) + MID * mass
        mask1 = plane_mask((planes - 2,) + tail, 2, low, high)
        mask2 = plane_mask((planes - 4,) + tail, 1, low, high)
        return basis_fields(wide_ref[slot, b], diag, mass, mask1, mask2)

    def one_source(b, carry):
        for k, field in enumerate(basis_of(group, b)):
            rounded = field.astype(jnp.bfloat16)
            raw_ref[b * BASIS + k] = rounded
            raw_ref[columns + b * BASIS + k] = (field - rounded.astype(jnp.float32)).astype(
                jnp.bfloat16
            )
        return carry

    for part in range(HALVES):
        settled(group, part)
        if part == HALVES - 1:
            for i in range(1, min(groups, 3)):
                pass_on(i)
            spread_planes(1)
        lax.fori_loop(part * half, (part + 1) * half, one_source, 0)
    fields_ref[...] = raw_ref[...].reshape(fields_ref.shape)

    def images_of(slot, part):
        def one(b, carry):
            w0, a0, a1, b0, b1, b2, e0, e1, e2, e3 = basis_of(slot, b)
            place = slot * nb + b
            image_ref[0, place] = w0
            for j in range(shifts):
                tau = table_ref[ids_ref[j]] - MID
                image_ref[1 + j, place] = a0 + tau * a1
                image_ref[1 + shifts + j, place] = b0 + tau * (b1 + tau * b2)
                image_ref[1 + 2 * shifts + j, place] = e0 + tau * (e1 + tau * (e2 + tau * e3))
            return carry

        lax.fori_loop(part * half, (part + 1) * half, one, 0)

    def scatter(u, there):
        turn = lax.rem(u, turns)
        return remote(
            out_buf.at[u, pl.ds(lax.rem(there, nb) * BASIS, BASIS)],
            in_buf.at[me, :, pl.ds(turn * parts, parts)],
            rs_send.at[u, lax.rem(there, nb)], rs_recv, dom=there,
        )

    def each_target(u, act):
        base = (u // turns) * nb
        for t in range(1, nb + 1):
            there = base + lax.rem(me + t, nb)

            @pl.when(there != me)
            def _(there=there):
                act(scatter(u, there))

    def step(u, carry):
        product = lax.dot_general(
            mat_ref[pl.ds(pl.multiple_of(u * stride, stride), stride)],
            fields_ref[...], (((1,), (1,)), ((), ())), preferred_element_type=jnp.float32,
        )
        turned = product.T
        summed = turned[:columns] + turned[columns:]
        for part in range(parts):
            out_buf[u, :, part, 0, :] = summed[:, part * LANES : (part + 1) * LANES]
        each_target(u, lambda copy: copy.start())
        return carry

    lax.fori_loop(0, steps - 1, step, 0)
    for i in range(3, groups):
        pass_on(i)
    lax.fori_loop(steps - 1, steps, step, 0)
    spread_planes(2)
    for part in range(HALVES):
        images_of(group, part)
    settled(other(1), 0)
    images_of(other(1), 0)

    first_turn = (me // nb) * turns
    mine = pl.ds(lax.rem(me, nb) * BASIS, BASIS)
    for turn in range(turns):
        in_buf[me, :, pl.ds(turn * parts, parts)] = out_buf[first_turn + turn, mine]
    remote(
        in_buf.at[pl.ds(0, n - 1)], in_buf.at[pl.ds(0, n - 1)], rs_send.at[0, 0], rs_recv, dom=right
    ).wait_recv()
    for k in range(BASIS):
        summed = in_buf[0, k]
        for source in range(1, n):
            summed = summed + in_buf[source, k]
        total_ref[k] = summed.reshape(total_ref.shape[1:])
    lane = lax.broadcasted_iota(jnp.int32, total_ref.shape[1:], 1)
    gram = jnp.zeros(total_ref.shape[1:], jnp.float32)
    for p, (i, k) in enumerate(PAIRS):
        value = jnp.sum(total_ref[i] * total_ref[k], axis=1, keepdims=True)
        gram = jnp.where(lane == p, value, gram)
    own = group * n + me
    gram_all[own] = jnp.sum(gram, axis=0, keepdims=True)

    def every(act):
        for dz in range(groups - 1, -1, -1):
            there = lax.rem(group + dz, groups)
            for dd in range(n):
                if dz or dd:
                    act(there, lax.rem(me + dd, n))

    def share(there, where):
        remote(
            gram_all.at[own], gram_all.at[own], g_send, g_recv, dom=where, shift=there
        ).start()

    others = gram_all.at[pl.ds(0, groups * n - 1)]
    everybody = remote(others, others, g_send, g_recv, dom=right)
    every(share)
    for i in range(3, groups):
        spread_planes(i)
    def sent(u, carry):
        each_target(u, lambda copy: copy.wait_send())
        return carry

    lax.fori_loop(0, steps, sent, 0)

    for i in range(groups):
        slot = other(i)

        @pl.when(up_from(slot))
        def _():
            for part in range(HALVES):
                across(slot, 0, part).wait_send()

        @pl.when(down_from(slot))
        def _():
            for part in range(HALVES):
                across(slot, 1, part).wait_send()

    settled(other(1), 1)
    images_of(other(1), 1)
    for i in range(2, groups):
        for part in range(HALVES):
            settled(other(i), part)
            images_of(other(i), part)

    everybody.wait_recv()
    for t in range(groups * n):
        gram_rows[t : t + 1] = gram_all[t]
    tau = jnp.zeros((1, LANES), jnp.float32)
    lane_row = lax.broadcasted_iota(jnp.int32, (1, LANES), 1)
    for j in range(shifts):
        tau = jnp.where(lane_row == j, table_ref[ids_ref[j]] - MID, tau)
    count = groups * nb
    grams = gram_rows[...]
    if n > nb:
        grams = jnp.sum(grams.reshape(groups, n // nb, nb, LANES), axis=1).reshape(count, LANES)
    for q, value in enumerate(weights(coefficients(grams, tau), tau)):
        for j in range(shifts):
            c_ref[q * shifts + j] = jnp.broadcast_to(value[:, j : j + 1], (count, LANES))

    @pl.when(has_right)
    def _():
        for i in range(groups):
            for part in range(HALVES):
                halo(other(i), 0, part).wait_send()
        for which in range(2):
            coeff_halo(which, 0).wait_send()

    @pl.when(has_left)
    def _():
        for i in range(groups):
            for part in range(HALVES):
                halo(other(i), 1, part).wait_send()
        for which in range(2):
            coeff_halo(which, 1).wait_send()

    everybody.wait_send()


def combine_kernel(image_ref, c_ref, sol_hbm, res_hbm, sol_ref, res_ref, sem):
    shifts, count = sol_ref.shape[0], sol_ref.shape[1]
    batch = count // sem.shape[1]

    def leave(k):
        part = pl.ds(k * batch, batch)
        return [
            pltpu.make_async_copy(here.at[:, part], there.at[:, part], sem.at[which, k])
            for which, (here, there) in enumerate(((sol_ref, sol_hbm), (res_ref, res_hbm)))
        ]

    def one_source(b, carry):
        w0 = image_ref[0, b]
        for j in range(shifts):
            z0 = image_ref[1 + j, b]
            z1 = image_ref[1 + shifts + j, b]
            z2 = image_ref[1 + 2 * shifts + j, b]
            of_w0, of_z0, of_z1, c0, c1, c2 = [
                c_ref[q * shifts + j, pl.ds(b, 1)] for q in range(WEIGHTS)
            ]
            sol_ref[j, b] = of_w0 * w0 + of_z0 * z0 + of_z1 * z1
            res_ref[j, b] = w0 - c0 * z0 - c1 * z1 - c2 * z2
        return carry

    def one_batch(k, carry):
        lax.fori_loop(k * batch, (k + 1) * batch, one_source, 0)
        for copy in leave(k):
            copy.start()
        return carry

    def gone(k, carry):
        for copy in leave(k):
            copy.wait()
        return carry

    lax.fori_loop(0, sem.shape[1], one_batch, 0)
    lax.fori_loop(0, sem.shape[1], gone, 0)


def on_device(sources, kappa, mass, shift_table, shift_ids, sketch):
    n, groups = lax.axis_size("dom"), lax.axis_size("shift")
    nb, slab = sources.shape[0], sources.shape[1]
    tail = sources.shape[2:]
    shifts = shift_ids.shape[0]
    rows = sketch.shape[0]
    block = rows // 8
    cells = slab * tail[0] * tail[1]
    planes = slab + 2 * HALO
    count = groups * nb
    columns = BASIS * nb
    stride = rows // STEPS
    parts = stride // LANES
    chunk = rows // (n // nb)
    turns = chunk // stride
    vmem = pl.BlockSpec(memory_space=pltpu.VMEM)
    hbm = pl.BlockSpec(memory_space=pl.ANY)
    smem = pl.BlockSpec(memory_space=pltpu.SMEM)
    dma = pltpu.SemaphoreType.DMA
    f32 = jnp.float32
    images, solved = pl.pallas_call(
        functools.partial(project_kernel, n, groups),
        out_shape=(
            pltpu.VMEM((1 + 3 * shifts, count, slab) + tail, f32),
            pltpu.VMEM((WEIGHTS * shifts, count, LANES), f32),
        ),
        in_specs=[hbm, hbm, hbm, smem, smem, hbm],
        out_specs=(vmem, vmem),
        scratch_shapes=[
            pltpu.VMEM((groups, nb, planes) + tail, f32),
            pltpu.VMEM((2, planes) + tail, f32),
            pltpu.VMEM((rows // block, block, slab) + tail, jnp.bfloat16),
            pltpu.VMEM((rows, cells), jnp.bfloat16),
            pltpu.VMEM((2 * columns, slab) + tail, jnp.bfloat16),
            pltpu.VMEM((2 * columns, cells), jnp.bfloat16),
            pltpu.VMEM((STEPS, columns, parts, 1, LANES), f32),
            pltpu.VMEM((n, BASIS, turns * parts, 1, LANES), f32),
            pltpu.VMEM((BASIS, turns * parts, LANES), f32),
            pltpu.VMEM((groups * n, 1, LANES), f32),
            pltpu.VMEM((groups * n, LANES), f32),
            dma((rows // block,)), dma((3,)),
            dma((groups, 2, HALVES)), dma((groups, HALVES)),
            dma((groups, 2, HALVES)), dma((groups, 2, HALVES)),
            dma((2, 2)), dma((2, 2)),
            dma((STEPS, nb)), dma,
            dma, dma,
        ],
        compiler_params=pltpu.CompilerParams(
            collective_id=0, has_side_effects=True, vmem_limit_bytes=46 << 20
        ),
        name="project",
    )(sources, kappa, mass, shift_table, shift_ids, sketch)

    batch = 2 if count % 2 == 0 else 1
    everything = (shifts, count, slab) + tail
    out = pltpu.HBM(everything, f32)
    return pl.pallas_call(
        combine_kernel,
        out_shape=(out, out),
        in_specs=[vmem, vmem],
        out_specs=(pl.BlockSpec(memory_space=pltpu.HBM),) * 2,
        scratch_shapes=[
            pltpu.VMEM(everything, f32),
            pltpu.VMEM(everything, f32),
            dma((2, count // batch)),
        ],
        compiler_params=pltpu.CompilerParams(vmem_limit_bytes=20 << 20),
        name="combine",
    )(
        pltpu.with_memory_space_constraint(images, pltpu.VMEM),
        pltpu.with_memory_space_constraint(solved, pltpu.VMEM),
    )


def solution(mesh):
    placed = (
        P("shift", "dom", None, None),
        P("dom", None, None),
        P("dom", None, None),
        P(),
        P("shift"),
        P(None, "dom", None, None),
    )
    return jax.shard_map(
        on_device,
        mesh=mesh,
        in_specs=placed,
        out_specs=(P("shift", None, "dom", None, None), P("shift", None, "dom", None, None)),
        check_vma=False,
    )
```
